32 devices in a mesh: samples: 8 (over z, y), variants: 4 (over x, core).
Axes of the slice: x: 2, y: 2, z: 4, core: 2. Of those that a mesh axis runs over, the one named last changes fastest.
Arguments:
- genotypes: int32 [2048, 32768], P('variants', 'samples'), may hold values from 0 to 3, as said below
- weights: float32 [32768], P('samples'), may hold values from 0.25 to 20
Outputs:
- call_mean: float32 [2048], P('variants')
- call_var: float32 [2048], P('variants')
- class_counts: int32 [4, 2048], P(None, 'variants')
- ld_window: float32 [1024, 2048], P('samples', 'variants')
- sample_calls: int32 [2, 32768], P(None, 'samples')
- sample_share: float32 [32768], P('samples')
The draws below stay inside these ranges and needn't reach their ends.
Inputs may be any that keep to these rules, and one draw needn't show every extreme that they name: `genotypes`: in every variant's row, each aligned group of 8 samples (samples 8 i to 8 i + 7) holds at least one call other than 3.
All inputs are finite; a program needn't handle non-finite values.
Results may differ from the reference program's by a relative error of at most 0.0004.
Values may be sent and summed in bfloat16 or wider, within the bound.
A program may use at most 64 MiB of HBM per device.

```python
import jax
import jax.numpy as jnp
from jax import lax

VAR_DEV = 512
VARIANTS = 2048
SAMPLES = 32768


def draw_genotypes(key, part):
    keys = jax.random.split(key, 6)
    level_all = jax.random.randint(keys[0], (VARIANTS,), 150, 500)
    hold_all = jax.random.randint(keys[1], (VARIANTS,), 300, 850)
    gap_all = jax.random.randint(keys[2], (VARIANTS,), 20, 400)
    step_keys = jax.random.split(keys[3], VARIANTS)
    slot = jnp.arange(SAMPLES, dtype=jnp.int32) % 8
    first_start = jax.random.randint(keys[4], (SAMPLES,), 0, 1000) < 300
    second_start = jax.random.randint(keys[5], (SAMPLES,), 0, 1000) < 300

    def advance(carry, inputs):
        first_hap, second_hap = carry
        step_key, level, hold, gap = inputs
        pieces = jax.random.split(step_key, 6)
        fresh_one = jax.random.randint(pieces[0], (SAMPLES,), 0, 1000) < level
        fresh_two = jax.random.randint(pieces[1], (SAMPLES,), 0, 1000) < level
        keep_one = jax.random.randint(pieces[2], (SAMPLES,), 0, 1000) < hold
        keep_two = jax.random.randint(pieces[3], (SAMPLES,), 0, 1000) < hold
        new_one = jnp.where(keep_one, first_hap, fresh_one)
        new_two = jnp.where(keep_two, second_hap, fresh_two)
        chosen = jnp.repeat(jax.random.randint(pieces[5], (SAMPLES // 8,), 0, 8), 8)
        lost = (jax.random.randint(pieces[4], (SAMPLES,), 0, 1000) < gap) & (slot != chosen)
        calls = jnp.where(lost, 3, new_one.astype(jnp.int32) + new_two.astype(jnp.int32))
        return ((new_one, new_two), calls.astype(jnp.int32))
    final_state, rows = lax.scan(advance, (first_start, second_start), (step_keys, level_all, hold_all, gap_all))
    return rows


def draw_weights(key, part):
    position = jnp.arange(SAMPLES, dtype=jnp.float32) / max(SAMPLES - 1, 1)
    base = jnp.exp(jax.random.uniform(key, (SAMPLES,), jnp.float32, jnp.log(0.3), jnp.log(3.0)))
    rise = 1.0 + 2.0 * position
    return (base * rise).astype(jnp.float32)


def setup_inputs(seed: int = 0) -> dict:
    key_list = jax.random.split(jax.random.key(seed), 3)
    genotypes = draw_genotypes(jax.random.fold_in(key_list[2], 71), 0)
    weights = draw_weights(jax.random.fold_in(key_list[2], 71), 0)
    return dict(genotypes=genotypes, weights=weights)


def reference(genotypes, weights):
    block_count = VARIANTS // VAR_DEV
    blocks = genotypes.reshape(block_count, VAR_DEV, SAMPLES)
    root_weight = jnp.sqrt(weights)

    def block_stats(block):
        present = block != 3
        called = present.astype(jnp.float32)
        dosage = jnp.where(present, block, 0).astype(jnp.float32)
        weighted = called * weights[None, :]
        w_sum = lax.optimization_barrier(jnp.sum(weighted, axis=1))
        mean_value = lax.optimization_barrier(jnp.sum(weighted * dosage, axis=1)) / w_sum
        centered = (dosage - mean_value[:, None]) * called
        var_value = lax.optimization_barrier(jnp.sum(weighted * centered * centered, axis=1)) / w_sum
        counts = jnp.stack([lax.optimization_barrier(jnp.sum((block == level).astype(jnp.int32), axis=1)) for level in range(4)])
        factor = 1.0 / jnp.sqrt(w_sum * (var_value + 1e-05))
        scaled = (root_weight[None, :] * centered * factor[:, None]).astype(jnp.bfloat16)
        return (mean_value, var_value, counts, scaled)
    mean_value, var_value, counts, scaled = lax.map(block_stats, blocks)
    padded = jnp.concatenate([scaled, jnp.zeros((1, VAR_DEV, SAMPLES), scaled.dtype)], axis=0)

    def window(index):
        own = lax.dynamic_index_in_dim(padded, index, 0, keepdims=False)
        after = lax.dynamic_index_in_dim(padded, index + 1, 0, keepdims=False)
        joined = jnp.concatenate([own, after], axis=0).astype(jnp.float32)
        return jnp.dot(joined, own.astype(jnp.float32).T, preferred_element_type=jnp.float32)
    ld_blocks = lax.map(window, jnp.arange(block_count, dtype=jnp.int32))
    ld_window = ld_blocks.transpose(1, 0, 2).reshape(2 * VAR_DEV, VARIANTS)

    def sample_block(block_pair):
        block, scaled_block = block_pair
        squares = scaled_block.astype(jnp.float32)
        return (lax.optimization_barrier(jnp.sum((block != 3).astype(jnp.int32), axis=0)), lax.optimization_barrier(jnp.sum((block == 1).astype(jnp.int32), axis=0)), lax.optimization_barrier(jnp.sum(squares * squares, axis=0)))
    called_rows, het_rows, square_rows = lax.map(sample_block, (blocks, scaled))
    sample_calls = jnp.stack([lax.optimization_barrier(jnp.sum(called_rows, axis=0)), lax.optimization_barrier(jnp.sum(het_rows, axis=0))])
    sample_share = lax.optimization_barrier(jnp.sum(square_rows, axis=0)) * (SAMPLES / VARIANTS)
    return (mean_value.reshape(VARIANTS), var_value.reshape(VARIANTS), counts.transpose(1, 0, 2).reshape(4, VARIANTS), ld_window, sample_calls, sample_share)
```

```python
import functools

import jax
import jax.numpy as jnp
from jax import lax
from jax.experimental import pallas as pl
from jax.experimental.pallas import tpu as pltpu
from jax.sharding import PartitionSpec as P

MESH = pl.DeviceIdType.MESH
F32 = jnp.float32
BF16 = jnp.bfloat16
LANES = 128
STEP = 16
SLAB = 512


def kernel(
    S,
    V,
    CH,
    gen_hbm,
    w_ref,
    stat_out,
    count_out,
    ld_out,
    call_out,
    share_out,
    gen,
    code,
    ncode,
    scaled,
    nscaled,
    part,
    rcv,
    wacc,
    cacc,
    sacc,
    qacc,
    root,
    gat,
    par,
    npar,
    colm,
    colf,
    smp,
    gen_sem,
    code_send,
    code_recv,
    stat_send,
    stat_recv,
    par_send,
    par_recv,
    rs_send,
    rs_recv,
    smp_send,
    smp_recv,
):
    s = lax.axis_index("samples")
    v = lax.axis_index("variants")
    rows, width = gen.shape
    R = 2 * rows // S
    H = S // 2
    NC = rows // CH
    blocks = width // LANES
    slabs = width // SLAB
    has_next = v < V - 1
    has_prev = v > 0

    def chunk_rows(c):
        return pl.ds(pl.multiple_of(c * CH, CH), CH)

    def load(k):
        c = lax.rem(k + s, NC)
        return pltpu.make_async_copy(
            gen_hbm.at[chunk_rows(c)], gen.at[chunk_rows(c)], gen_sem.at[c]
        )

    def start_load(k, _):
        load(k).start()
        return 0

    lax.fori_loop(0, NC, start_load, 0)

    barrier = pltpu.get_barrier_semaphore()

    def greet_samples(d, _):
        pl.semaphore_signal(
            barrier,
            inc=1,
            device_id={"samples": lax.rem(s + d, S)},
            device_id_type=MESH,
        )
        return 0

    def greet_variants(d, _):
        pl.semaphore_signal(
            barrier,
            inc=1,
            device_id={"variants": lax.rem(v + d, V)},
            device_id_type=MESH,
        )
        return 0

    lax.fori_loop(1, S, greet_samples, 0)
    lax.fori_loop(1, V, greet_variants, 0)

    root[...] = jnp.sqrt(w_ref[...])
    sacc[...] = jnp.zeros_like(sacc)
    qacc[...] = jnp.zeros_like(qacc)

    def code_copy(c):
        return pltpu.make_async_remote_copy(
            src_ref=code.at[chunk_rows(c)],
            dst_ref=ncode.at[chunk_rows(c)],
            send_sem=code_send.at[c],
            recv_sem=code_recv.at[c],
            device_id={"variants": lax.rem(v + V - 1, V)},
            device_id_type=MESH,
        )

    def first_pass(k, _):
        c = lax.rem(k + s, NC)
        load(k).wait()

        def sixteen(i, _):
            here = pl.ds(pl.multiple_of(c * CH + i * STEP, STEP), STEP)
            zero = jnp.zeros((STEP, LANES), F32)
            w0, w1, w2 = zero, zero, zero
            cnt = jnp.zeros((STEP, LANES), jnp.int32)
            for b in range(blocks):
                lane = slice(b * LANES, (b + 1) * LANES)
                g = gen[here, lane]
                w = jnp.broadcast_to(w_ref[0:1, lane], (STEP, LANES))
                w0 = w0 + jnp.where(g == 0, w, 0.0)
                w1 = w1 + jnp.where(g == 1, w, 0.0)
                w2 = w2 + jnp.where(g == 2, w, 0.0)
                tag = jnp.left_shift(jnp.int32(1), jnp.left_shift(g, 3))
                cnt = cnt + tag
                sacc[:, lane] += tag[:8] + tag[8:]
                code[here, lane] = g.astype(F32).astype(BF16)
            wacc[0, here] = w0
            wacc[1, here] = w1
            wacc[2, here] = w2
            cacc[here] = cnt
            return 0

        lax.fori_loop(0, CH // STEP, sixteen, 0)

        @pl.when(k == 0)
        def _():
            pl.semaphore_wait(barrier, S + V - 2)

        @pl.when(has_prev)
        def _():
            code_copy(c).start()

        return 0

    lax.fori_loop(0, NC, first_pass, 0)

    def total(x):
        return jnp.sum(x.T, axis=0, keepdims=True)

    cnt = cacc[...]
    lines = [total(wacc[i]) for i in range(3)]
    for level in range(4):
        lines.append(
            total(jnp.bitwise_and(jnp.right_shift(cnt, 8 * level), 255).astype(F32))
        )
    lines.append(jnp.zeros_like(lines[0]))
    gat[s] = jnp.concatenate(lines, axis=0)

    def stat_copy(d, slot):
        return pltpu.make_async_remote_copy(
            src_ref=gat.at[slot],
            dst_ref=gat.at[slot],
            send_sem=stat_send.at[d],
            recv_sem=stat_recv.at[slot],
            device_id={"samples": lax.rem(s + d, S)},
            device_id_type=MESH,
        )

    def send_stat(d, _):
        stat_copy(d, s).start()
        return 0

    lax.fori_loop(1, S, send_stat, 0)

    def wait_stat(d, _):
        stat_copy(d, lax.rem(s + d, S)).wait_recv()
        return 0

    lax.fori_loop(1, S, wait_stat, 0)
    sums = gat[0]
    for t in range(1, S):
        sums = sums + gat[t]
    w0, w1, w2 = sums[0:1], sums[1:2], sums[2:3]
    w_sum = w0 + w1 + w2
    mean = (w1 + 2.0 * w2) / w_sum
    one, two = 1.0 - mean, 2.0 - mean
    var = (w0 * mean * mean + w1 * one * one + w2 * two * two) / w_sum
    factor = 1.0 / jnp.sqrt(w_sum * (var + 1e-05))
    stat_out[...] = jnp.concatenate([mean, var], axis=0)
    count_out[...] = sums[3:7].astype(jnp.int32)
    par[...] = jnp.concatenate([mean, factor, jnp.zeros((6, rows), F32)], axis=0)

    par_copy = pltpu.make_async_remote_copy(
        src_ref=par,
        dst_ref=npar,
        send_sem=par_send.at[0],
        recv_sem=par_recv.at[0],
        device_id={"variants": lax.rem(v + V - 1, V)},
        device_id_type=MESH,
    )

    @pl.when(has_prev)
    def _():
        par_copy.start()

    def columns(ref):
        turned = ref[...].T
        colm[...] = jnp.broadcast_to(turned[:, 0:1], colm.shape)
        colf[...] = jnp.broadcast_to(turned[:, 1:2], colf.shape)

    def scale(src, src_row, dst, dst_row, count, squares):
        def sixteen(i, _):
            here = pl.ds(pl.multiple_of(src_row + i * STEP, STEP), STEP)
            there = pl.ds(pl.multiple_of(dst_row + i * STEP, STEP), STEP)
            m, f = colm[here], colf[here]
            for b in range(blocks):
                lane = slice(b * LANES, (b + 1) * LANES)
                d = src[here, lane].astype(F32)
                r = jnp.broadcast_to(root[0:1, lane], (STEP, LANES))
                x = jnp.where(d < 2.5, r * (d - m) * f, 0.0).astype(BF16)
                dst[there, lane] = x
                if squares:
                    y = x.astype(F32)
                    y = y * y
                    qacc[:, lane] += y[:8] + y[8:]
            return 0

        lax.fori_loop(0, count // STEP, sixteen, 0)

    columns(par)
    scale(code, 0, scaled, 0, rows, True)

    def rs_copy(owner, slot):
        return pltpu.make_async_remote_copy(
            src_ref=part.at[owner],
            dst_ref=rcv.at[slot],
            send_sem=rs_send.at[owner],
            recv_sem=rs_recv.at[slot],
            device_id={"samples": owner},
            device_id_type=MESH,
        )

    def correlate(left):
        return lax.dot_general(
            left, scaled[...], (((1,), (1,)), ((), ())), preferred_element_type=F32
        )

    def own_rows(k, _):
        owner = lax.rem(s + k, H)
        rows_here = pl.ds(pl.multiple_of(owner * R, R), R)
        part[owner] = correlate(scaled[rows_here, :])

        @pl.when(owner != s)
        def _():
            rs_copy(owner, s).start()

        return 0

    lax.fori_loop(0, H, own_rows, 0)

    packed = sacc[...]
    tags = [
        jnp.bitwise_and(jnp.right_shift(packed, 8 * level), 255).astype(F32)
        for level in range(3)
    ]
    for q, value in enumerate([tags[0] + tags[1] + tags[2], tags[1], qacc[...]]):
        line = jnp.sum(value, axis=0, keepdims=True)
        for i in range(slabs):
            smp[v, pl.ds(q * slabs + i, 1), :] = line[:, i * SLAB : (i + 1) * SLAB]

    def smp_copy(d, slot):
        return pltpu.make_async_remote_copy(
            src_ref=smp.at[slot],
            dst_ref=smp.at[slot],
            send_sem=smp_send.at[d],
            recv_sem=smp_recv.at[slot],
            device_id={"variants": lax.rem(v + d, V)},
            device_id_type=MESH,
        )

    def send_smp(d, _):
        smp_copy(d, v).start()
        return 0

    lax.fori_loop(1, V, send_smp, 0)

    @pl.when(has_next)
    def _():
        par_copy.wait_recv()
        columns(npar)

        def cross(k, _):
            c = lax.rem(k + s, NC)
            code_copy(c).wait_recv()
            scale(ncode, c * CH, nscaled, 0, CH, False)
            got = correlate(nscaled[...])
            for i in range(CH // R):
                owner = H + c * (CH // R) + i
                part[owner] = got[i * R : (i + 1) * R]

                @pl.when(owner != s)
                def _():
                    rs_copy(owner, s).start()

            return 0

        lax.fori_loop(0, NC, cross, 0)

    def wait_smp(d, _):
        smp_copy(d, lax.rem(v + d, V)).wait_recv()
        return 0

    lax.fori_loop(1, V, wait_smp, 0)
    all_sums = smp[0]
    for t in range(1, V):
        all_sums = all_sums + smp[t]
    call_out[...] = all_sums[: 2 * slabs].astype(jnp.int32)
    share_out[...] = all_sums[2 * slabs :] * F32((width * S) / (rows * V))

    sent_to_me = jnp.logical_or(s < H, has_next)

    @pl.when(sent_to_me)
    def _():
        ld_out[...] = part[s]

        def gather(d, _):
            t = lax.rem(s + d, S)
            rs_copy(s, t).wait_recv()
            ld_out[...] += rcv[t]
            return 0

        lax.fori_loop(1, S, gather, 0)

    @pl.when(jnp.logical_not(sent_to_me))
    def _():
        ld_out[...] = jnp.zeros_like(ld_out)

    def drain_samples(d, _):
        stat_copy(d, s).wait_send()
        owner = lax.rem(s + d, S)

        @pl.when(jnp.logical_or(owner < H, has_next))
        def _():
            rs_copy(owner, s).wait_send()

        return 0

    lax.fori_loop(1, S, drain_samples, 0)

    def drain_variants(d, _):
        smp_copy(d, v).wait_send()
        return 0

    lax.fori_loop(1, V, drain_variants, 0)

    @pl.when(has_prev)
    def _():
        par_copy.wait_send()

        def drain_codes(c, _):
            code_copy(c).wait_send()
            return 0

        lax.fori_loop(0, NC, drain_codes, 0)


def on_device(S, V, genotypes, weights):
    rows, width = genotypes.shape
    R = 2 * rows // S
    CH = max(128, R)
    NC = rows // CH
    slabs = width // SLAB
    vmem = pl.BlockSpec(memory_space=pltpu.VMEM)
    dma = pltpu.SemaphoreType.DMA
    stats, counts, ld, calls, share = pl.pallas_call(
        functools.partial(kernel, S, V, CH),
        out_shape=(
            jax.ShapeDtypeStruct((2, rows), F32),
            jax.ShapeDtypeStruct((4, rows), jnp.int32),
            jax.ShapeDtypeStruct((R, rows), F32),
            jax.ShapeDtypeStruct((2 * slabs, SLAB), jnp.int32),
            jax.ShapeDtypeStruct((slabs, SLAB), F32),
        ),
        in_specs=[pl.BlockSpec(memory_space=pl.ANY), vmem],
        out_specs=(vmem,) * 5,
        scratch_shapes=[
            pltpu.VMEM((rows, width), jnp.int32),
            pltpu.VMEM((rows, width), BF16),
            pltpu.VMEM((rows, width), BF16),
            pltpu.VMEM((rows, width), BF16),
            pltpu.VMEM((CH, width), BF16),
            pltpu.VMEM((S, R, rows), F32),
            pltpu.VMEM((S, R, rows), F32),
            pltpu.VMEM((3, rows, LANES), F32),
            pltpu.VMEM((rows, LANES), jnp.int32),
            pltpu.VMEM((8, width), jnp.int32),
            pltpu.VMEM((8, width), F32),
            pltpu.VMEM((1, width), F32),
            pltpu.VMEM((S, 8, rows), F32),
            pltpu.VMEM((8, rows), F32),
            pltpu.VMEM((8, rows), F32),
            pltpu.VMEM((rows, LANES), F32),
            pltpu.VMEM((rows, LANES), F32),
            pltpu.VMEM((V, 3 * slabs, SLAB), F32),
            dma((NC,)),
            dma((NC,)),
            dma((NC,)),
            dma((S,)),
            dma((S,)),
            dma((1,)),
            dma((1,)),
            dma((S,)),
            dma((S,)),
            dma((V,)),
            dma((V,)),
        ],
        compiler_params=pltpu.CompilerParams(
            collective_id=0, has_side_effects=True, vmem_limit_bytes=60 * 1024 * 1024
        ),
        name="window_stats",
    )(genotypes, weights.reshape(1, width))
    return (
        stats[0],
        stats[1],
        counts,
        ld,
        calls.reshape(2, width),
        share.reshape(width),
    )


def solution(mesh):
    body = functools.partial(on_device, mesh.shape["samples"], mesh.shape["variants"])
    return jax.shard_map(
        body,
        mesh=mesh,
        in_specs=(P("variants", "samples"), P("samples")),
        out_specs=(
            P("variants"),
            P("variants"),
            P(None, "variants"),
            P("samples", "variants"),
            P(None, "samples"),
            P("samples"),
        ),
        check_vma=False,
    )
```

```python
import functools

import jax
import jax.numpy as jnp
from jax import lax
from jax.experimental import pallas as pl
from jax.experimental.pallas import tpu as pltpu
from jax.sharding import PartitionSpec as P

MESH = pl.DeviceIdType.MESH
F32 = jnp.float32
BF16 = jnp.bfloat16
LANES = 128
STEP = 16
SUB = 32
FULL = 32400.0
SLAB = 512


def kernel(
    S,
    V,
    CH,
    gen_hbm,
    w_ref,
    stat_out,
    count_out,
    ld_out,
    call_out,
    share_out,
    gen,
    code,
    ncode,
    scaled,
    nscaled,
    part,
    mine,
    rcv,
    wacc,
    cacc,
    sacc,
    qacc,
    root,
    gat,
    ngat,
    par,
    colm,
    colf,
    cole,
    tall,
    ntall,
    smp,
    gen_sem,
    code_send,
    code_recv,
    stat_send,
    stat_recv,
    par_send,
    par_recv,
    rs_send,
    rs_recv,
    smp_send,
    smp_recv,
):
    s = lax.axis_index("samples")
    v = lax.axis_index("variants")
    rows, width = gen.shape
    R = 2 * rows // S
    H = S // 2
    NC = rows // CH
    blocks = width // LANES
    slabs = width // SLAB
    has_next = v < V - 1
    has_prev = v > 0

    def chunk_rows(c):
        return pl.ds(pl.multiple_of(c * CH, CH), CH)

    def load(k):
        c = lax.rem(k + s, NC)
        return pltpu.make_async_copy(
            gen_hbm.at[chunk_rows(c)], gen.at[chunk_rows(c)], gen_sem.at[c]
        )

    def start_load(k, _):
        load(k).start()
        return 0

    lax.fori_loop(0, NC, start_load, 0)

    barrier = pltpu.get_barrier_semaphore()

    def greet_samples(d, _):
        pl.semaphore_signal(
            barrier,
            inc=1,
            device_id={"samples": lax.rem(s + d, S)},
            device_id_type=MESH,
        )
        return 0

    def greet_variants(d, _):
        pl.semaphore_signal(
            barrier,
            inc=1,
            device_id={"variants": lax.rem(v + d, V)},
            device_id_type=MESH,
        )
        return 0

    lax.fori_loop(1, S, greet_samples, 0)
    lax.fori_loop(1, V, greet_variants, 0)

    root[...] = jnp.sqrt(w_ref[...])
    sacc[...] = jnp.zeros_like(sacc)
    qacc[...] = jnp.zeros_like(qacc)

    def code_copy(c):
        return pltpu.make_async_remote_copy(
            src_ref=code.at[chunk_rows(c)],
            dst_ref=ncode.at[chunk_rows(c)],
            send_sem=code_send.at[c],
            recv_sem=code_recv.at[c],
            device_id={"variants": lax.rem(v + V - 1, V)},
            device_id_type=MESH,
        )

    def piece_copy(c, h):
        here = pl.ds(pl.multiple_of(c * CH + h * SUB, SUB), SUB)
        return pltpu.make_async_remote_copy(
            src_ref=code.at[here],
            dst_ref=ncode.at[here],
            send_sem=code_send.at[c],
            recv_sem=code_recv.at[c],
            device_id={"variants": lax.rem(v + V - 1, V)},
            device_id_type=MESH,
        )

    def first_pass(k, _):
        c = lax.rem(k + s, NC)
        load(k).wait()

        def sixteen(i, _):
            here = pl.ds(pl.multiple_of(c * CH + i * STEP, STEP), STEP)
            zero = jnp.zeros((STEP, LANES), F32)
            w0, w1, w2 = zero, zero, zero
            cnt = jnp.zeros((STEP, LANES), jnp.int32)
            for b in range(blocks):
                lane = slice(b * LANES, (b + 1) * LANES)
                g = gen[here, lane]
                w = jnp.broadcast_to(w_ref[0:1, lane], (STEP, LANES))
                w0 = w0 + jnp.where(g == 0, w, 0.0)
                w1 = w1 + jnp.where(g == 1, w, 0.0)
                w2 = w2 + jnp.where(g == 2, w, 0.0)
                tag = jnp.left_shift(jnp.int32(1), jnp.left_shift(g, 3))
                cnt = cnt + tag
                sacc[:, lane] += tag[:8] + tag[8:]
                code[here, lane] = g.astype(F32).astype(BF16)
            wacc[0, here] = w0
            wacc[1, here] = w1
            wacc[2, here] = w2
            cacc[here] = cnt
            return 0

        def piece(h, _):
            lax.fori_loop(h * (SUB // STEP), (h + 1) * (SUB // STEP), sixteen, 0)

            @pl.when(jnp.logical_and(k == 0, h == 0))
            def _():
                pl.semaphore_wait(barrier, S + V - 2)

            @pl.when(has_prev)
            def _():
                piece_copy(c, h).start()

            return 0

        lax.fori_loop(0, CH // SUB, piece, 0)
        return 0

    lax.fori_loop(0, NC, first_pass, 0)

    def total(x):
        return jnp.sum(x.T, axis=0, keepdims=True)

    cnt = cacc[...]
    lines = [total(wacc[i]) for i in range(3)]
    for level in range(4):
        lines.append(
            total(jnp.bitwise_and(jnp.right_shift(cnt, 8 * level), 255).astype(F32))
        )
    lines.append(jnp.zeros_like(lines[0]))
    gat[s] = jnp.concatenate(lines, axis=0)

    def stat_copy(d, slot):
        return pltpu.make_async_remote_copy(
            src_ref=gat.at[slot],
            dst_ref=gat.at[slot],
            send_sem=stat_send.at[d],
            recv_sem=stat_recv.at[slot],
            device_id={"samples": lax.rem(s + d, S)},
            device_id_type=MESH,
        )

    def send_stat(d, _):
        stat_copy(d, s).start()
        return 0

    lax.fori_loop(1, S, send_stat, 0)

    def wait_stat(d, _):
        stat_copy(d, lax.rem(s + d, S)).wait_recv()
        return 0

    lax.fori_loop(1, S, wait_stat, 0)

    def moments(ref):
        sums = ref[0]
        for t in range(1, S):
            sums = sums + ref[t]
        w0, w1, w2 = sums[0:1], sums[1:2], sums[2:3]
        w_sum = w0 + w1 + w2
        mean = (w1 + 2.0 * w2) / w_sum
        one, two = 1.0 - mean, 2.0 - mean
        var = (w0 * mean * mean + w1 * one * one + w2 * two * two) / w_sum
        factor = 1.0 / jnp.sqrt(w_sum * (var + 1e-05))
        return sums, mean, var, factor

    def norm(ref, t, mean, factor):
        w0, w1, w2 = ref[t, 0:1], ref[t, 1:2], ref[t, 2:3]
        one, two = 1.0 - mean, 2.0 - mean
        length = jnp.sqrt(w0 * mean * mean + w1 * one * one + w2 * two * two)
        return jnp.maximum(length * factor, 1e-12)

    par_copy = pltpu.make_async_remote_copy(
        src_ref=gat,
        dst_ref=ngat,
        send_sem=par_send.at[0],
        recv_sem=par_recv.at[0],
        device_id={"variants": lax.rem(v + V - 1, V)},
        device_id_type=MESH,
    )

    @pl.when(has_prev)
    def _():
        par_copy.start()

    sums, mean, var, factor = moments(gat)
    stat_out[...] = jnp.concatenate([mean, var], axis=0)
    count_out[...] = sums[3:7].astype(jnp.int32)
    level = FULL / norm(gat, s, mean, factor)

    def columns(ref, mean, factor, turned_norms):
        mine_now = FULL / norm(ref, s, mean, factor)
        par[...] = jnp.concatenate(
            [mean, factor, mine_now, jnp.zeros((5, rows), F32)], axis=0
        )
        turned = par[...].T
        colm[...] = jnp.broadcast_to(turned[:, 0:1], colm.shape)
        colf[...] = jnp.broadcast_to(turned[:, 1:2], colf.shape)
        cole[...] = jnp.broadcast_to(turned[:, 2:3], cole.shape)
        every = jnp.concatenate([norm(ref, t, mean, factor) for t in range(S)], axis=0)
        turned_norms[:, 0:S] = every.T

    def scale(src, src_row, dst, dst_row, count, squares):
        def sixteen(i, _):
            here = pl.ds(pl.multiple_of(src_row + i * STEP, STEP), STEP)
            there = pl.ds(pl.multiple_of(dst_row + i * STEP, STEP), STEP)
            m, f = colm[here], colf[here]
            for b in range(blocks):
                lane = slice(b * LANES, (b + 1) * LANES)
                d = src[here, lane].astype(F32)
                r = jnp.broadcast_to(root[0:1, lane], (STEP, LANES))
                x = jnp.where(d < 2.5, r * (d - m) * f, 0.0).astype(BF16)
                dst[there, lane] = x
                if squares:
                    y = x.astype(F32)
                    y = y * y
                    qacc[:, lane] += y[:8] + y[8:]
            return 0

        lax.fori_loop(0, count // STEP, sixteen, 0)

    columns(gat, mean, factor, tall)
    scale(code, 0, scaled, 0, rows, True)

    def rs_copy(owner, slot):
        return pltpu.make_async_remote_copy(
            src_ref=part.at[owner],
            dst_ref=rcv.at[slot],
            send_sem=rs_send.at[owner],
            recv_sem=rs_recv.at[slot],
            device_id={"samples": owner},
            device_id_type=MESH,
        )

    def correlate(left):
        return lax.dot_general(
            left, scaled[...], (((1,), (1,)), ((), ())), preferred_element_type=F32
        )

    level_row = level * (1.0 / FULL)

    def hand_over(value, owner, row):
        e = cole[pl.ds(pl.multiple_of(row, R), R), 0:1]

        @pl.when(owner == s)
        def _():
            mine[...] = value

        @pl.when(owner != s)
        def _():
            q = jnp.round(value * e * level_row)
            q = jnp.clip(q, -32767.0, 32767.0)
            part[owner] = q.astype(jnp.int32).astype(jnp.int16)
            rs_copy(owner, s).start()

    def own_rows(k, _):
        owner = lax.rem(s + k, H)
        rows_here = pl.ds(pl.multiple_of(owner * R, R), R)
        hand_over(correlate(scaled[rows_here, :]), owner, owner * R)

        return 0

    lax.fori_loop(0, H, own_rows, 0)

    packed = sacc[...]
    tags = [
        jnp.bitwise_and(jnp.right_shift(packed, 8 * level), 255).astype(F32)
        for level in range(3)
    ]
    for q, value in enumerate([tags[0] + tags[1] + tags[2], tags[1], qacc[...]]):
        line = jnp.sum(value, axis=0, keepdims=True)
        for i in range(slabs):
            smp[v, pl.ds(q * slabs + i, 1), :] = line[:, i * SLAB : (i + 1) * SLAB]

    def smp_copy(d, slot):
        return pltpu.make_async_remote_copy(
            src_ref=smp.at[slot],
            dst_ref=smp.at[slot],
            send_sem=smp_send.at[d],
            recv_sem=smp_recv.at[slot],
            device_id={"variants": lax.rem(v + d, V)},
            device_id_type=MESH,
        )

    def send_smp(d, _):
        smp_copy(d, v).start()
        return 0

    lax.fori_loop(1, V, send_smp, 0)

    @pl.when(has_next)
    def _():
        par_copy.wait_recv()
        _, nmean, _, nfactor = moments(ngat)
        columns(ngat, nmean, nfactor, ntall)

        def cross(k, _):
            c = lax.rem(k + s, NC)
            code_copy(c).wait_recv()
            scale(ncode, c * CH, nscaled, 0, CH, False)
            got = correlate(nscaled[...])
            for i in range(CH // R):
                owner = H + c * (CH // R) + i
                hand_over(got[i * R : (i + 1) * R], owner, c * CH + i * R)

            return 0

        lax.fori_loop(0, NC, cross, 0)

    def wait_smp(d, _):
        smp_copy(d, lax.rem(v + d, V)).wait_recv()
        return 0

    lax.fori_loop(1, V, wait_smp, 0)
    all_sums = smp[0]
    for t in range(1, V):
        all_sums = all_sums + smp[t]
    call_out[...] = all_sums[: 2 * slabs].astype(jnp.int32)
    share_out[...] = all_sums[2 * slabs :] * F32((width * S) / (rows * V))

    sent_to_me = jnp.logical_or(s < H, has_next)

    def gather(norms, row):
        ld_out[...] = mine[...]
        for t in range(S):

            @pl.when(t != s)
            def _():
                rs_copy(s, t).wait_recv()
                col = norm(gat, t, mean, factor) * (1.0 / FULL)
                e = norms[pl.ds(pl.multiple_of(row, R), R), t : t + 1]
                ld_out[...] += rcv[t].astype(jnp.int32).astype(F32) * e * col

    @pl.when(s < H)
    def _():
        gather(tall, s * R)

    @pl.when(jnp.logical_and(s >= H, has_next))
    def _():
        gather(ntall, (s - H) * R)

    @pl.when(jnp.logical_not(sent_to_me))
    def _():
        ld_out[...] = jnp.zeros_like(ld_out)

    def drain_samples(d, _):
        stat_copy(d, s).wait_send()
        owner = lax.rem(s + d, S)

        @pl.when(jnp.logical_or(owner < H, has_next))
        def _():
            rs_copy(owner, s).wait_send()

        return 0

    lax.fori_loop(1, S, drain_samples, 0)

    def drain_variants(d, _):
        smp_copy(d, v).wait_send()
        return 0

    lax.fori_loop(1, V, drain_variants, 0)

    @pl.when(has_prev)
    def _():
        par_copy.wait_send()

        def drain_codes(c, _):
            code_copy(c).wait_send()
            return 0

        lax.fori_loop(0, NC, drain_codes, 0)


def finish(stats, counts, ld, calls, share, mean, var, counts_o, ld_o, calls_o, share_o):
    slabs = share.shape[0]
    mean[...] = stats[0]
    var[...] = stats[1]
    counts_o[...] = counts[...]
    ld_o[...] = ld[...]
    for i in range(slabs):
        here = slice(i * SLAB, (i + 1) * SLAB)
        for q in range(2):
            calls_o[q : q + 1, here] = calls[q * slabs + i : q * slabs + i + 1]
        share_o[here] = share[i]


def on_device(S, V, genotypes, weights):
    rows, width = genotypes.shape
    R = 2 * rows // S
    CH = max(128, R)
    NC = rows // CH
    slabs = width // SLAB
    vmem = pl.BlockSpec(memory_space=pltpu.VMEM)
    dma = pltpu.SemaphoreType.DMA
    stats, counts, ld, calls, share = pl.pallas_call(
        functools.partial(kernel, S, V, CH),
        out_shape=(
            jax.ShapeDtypeStruct((2, rows), F32),
            jax.ShapeDtypeStruct((4, rows), jnp.int32),
            jax.ShapeDtypeStruct((R, rows), F32),
            jax.ShapeDtypeStruct((2 * slabs, SLAB), jnp.int32),
            jax.ShapeDtypeStruct((slabs, SLAB), F32),
        ),
        in_specs=[pl.BlockSpec(memory_space=pl.ANY), vmem],
        out_specs=(vmem,) * 5,
        scratch_shapes=[
            pltpu.VMEM((rows, width), jnp.int32),
            pltpu.VMEM((rows, width), BF16),
            pltpu.VMEM((rows, width), BF16),
            pltpu.VMEM((rows, width), BF16),
            pltpu.VMEM((CH, width), BF16),
            pltpu.VMEM((S, R, rows), jnp.int16),
            pltpu.VMEM((R, rows), F32),
            pltpu.VMEM((S, R, rows), jnp.int16),
            pltpu.VMEM((3, rows, LANES), F32),
            pltpu.VMEM((rows, LANES), jnp.int32),
            pltpu.VMEM((8, width), jnp.int32),
            pltpu.VMEM((8, width), F32),
            pltpu.VMEM((1, width), F32),
            pltpu.VMEM((S, 8, rows), F32),
            pltpu.VMEM((S, 8, rows), F32),
            pltpu.VMEM((8, rows), F32),
            pltpu.VMEM((rows, LANES), F32),
            pltpu.VMEM((rows, LANES), F32),
            pltpu.VMEM((rows, LANES), F32),
            pltpu.VMEM((rows, LANES), F32),
            pltpu.VMEM((rows, LANES), F32),
            pltpu.VMEM((V, 3 * slabs, SLAB), F32),
            dma((NC,)),
            dma((NC,)),
            dma((NC,)),
            dma((S,)),
            dma((S,)),
            dma((1,)),
            dma((1,)),
            dma((S,)),
            dma((S,)),
            dma((V,)),
            dma((V,)),
        ],
        compiler_params=pltpu.CompilerParams(
            collective_id=0, has_side_effects=True, vmem_limit_bytes=60 * 1024 * 1024
        ),
        name="window_stats",
    )(genotypes, weights.reshape(1, width))
    return pl.pallas_call(
        finish,
        out_shape=(
            jax.ShapeDtypeStruct((rows,), F32),
            jax.ShapeDtypeStruct((rows,), F32),
            jax.ShapeDtypeStruct((4, rows), jnp.int32),
            jax.ShapeDtypeStruct((R, rows), F32),
            jax.ShapeDtypeStruct((2, width), jnp.int32),
            jax.ShapeDtypeStruct((width,), F32),
        ),
        in_specs=[vmem] * 5,
        out_specs=(vmem,) * 6,
        name="finish",
    )(stats, counts, ld, calls, share)


def solution(mesh):
    body = functools.partial(on_device, mesh.shape["samples"], mesh.shape["variants"])
    return jax.shard_map(
        body,
        mesh=mesh,
        in_specs=(P("variants", "samples"), P("samples")),
        out_specs=(
            P("variants"),
            P("variants"),
            P(None, "variants"),
            P("samples", "variants"),
            P(None, "samples"),
            P("samples"),
        ),
        check_vma=False,
    )
```
